32 devices in a mesh: dp: 2 (over y), mp: 4 (over z), expert: 4 (over x, core).
Axes of the slice: x: 2, y: 2, z: 4, core: 2. Of those that a mesh axis runs over, the one named last changes fastest.
Arguments:
- layer_input: bfloat16 [8, 1024, 2048], P(('dp', 'expert'), 'mp'), may hold values from -7 to 7
- w_query: bfloat16 [2048, 3072], P(('dp', 'expert'), 'mp'), may hold values from -1 to 1
- w_latent: bfloat16 [2048, 576], P(('dp', 'mp', 'expert')), may hold values from -1 to 1
- latent_gain: float32 [512], replicated, may hold values from 0.5 to 1.5
- w_expand: bfloat16 [512, 4096], P(('dp', 'expert'), 'mp'), may hold values from -1 to 1
- w_output: bfloat16 [2048, 2048], P('mp', ('dp', 'expert')), may hold values from -0.75 to 0.75
- attn_gain: float32 [2048], replicated, may hold values from 0.5 to 1.5
- ffn_gain: float32 [2048], replicated, may hold values from 0.5 to 1.5
- shared_gate: bfloat16 [2048, 2816], P(('dp', 'expert'), 'mp'), may hold values from -0.125 to 0.125
- shared_up: bfloat16 [2048, 2816], P(('dp', 'expert'), 'mp'), may hold values from -0.125 to 0.125
- shared_down: bfloat16 [2816, 2048], P('mp', ('dp', 'expert')), may hold values from -0.109375 to 0.109375
- expert_gate: bfloat16 [16, 2048, 1408], P(('mp', 'expert'), 'dp'), may hold values from -0.125 to 0.125
- expert_up: bfloat16 [16, 2048, 1408], P(('mp', 'expert'), 'dp'), may hold values from -0.125 to 0.125
- expert_down: bfloat16 [16, 1408, 2048], P(('mp', 'expert'), None, 'dp'), may hold values from -0.15625 to 0.15625
- routes: int32 [8, 1024, 6], P(('dp', 'expert'), 'mp'), may hold values from 0 to 15, all different within a row; in each aligned block of 256 rows (0 to 255, 256 to 511, ..., all dimensions but the last counted through in order) at most 192 rows name the same one
- combine: float32 [8, 1024, 6], P(('dp', 'expert'), 'mp'), may hold values from 0.05 to 0.4
- cotangent: bfloat16 [8, 1024, 2048], P(('dp', 'expert'), 'mp'), may hold values from -6 to 6
Outputs:
- layer_output: float32 [8, 1024, 2048], P(('dp', 'expert'), 'mp')
- d_layer_input: float32 [8, 1024, 2048], P(('dp', 'expert'), 'mp')
- d_w_query: float32 [2048, 3072], P(('dp', 'expert'), 'mp')
- d_w_latent: float32 [2048, 576], P(('dp', 'mp', 'expert'))
- d_latent_gain: float32 [512], replicated
- d_w_expand: float32 [512, 4096], P(('dp', 'expert'), 'mp')
- d_w_output: float32 [2048, 2048], P('mp', ('dp', 'expert'))
- d_attn_gain: float32 [2048], replicated
- d_ffn_gain: float32 [2048], replicated
- d_shared_gate: float32 [2048, 2816], P(('dp', 'expert'), 'mp')
- d_shared_up: float32 [2048, 2816], P(('dp', 'expert'), 'mp')
- d_shared_down: float32 [2816, 2048], P('mp', ('dp', 'expert'))
- d_expert_gate: float32 [16, 2048, 1408], P(('mp', 'expert'), 'dp')
- d_expert_up: float32 [16, 2048, 1408], P(('mp', 'expert'), 'dp')
- d_expert_down: float32 [16, 1408, 2048], P(('mp', 'expert'), None, 'dp')
The draws below stay inside these ranges and needn't reach their ends.
Inputs may be any that keep to these rules, and one draw needn't show every extreme that they name: `routes`: each token names 6 different experts. In the rows of one device (aligned blocks of 256 tokens) no expert is named by more than 192 of the (token, choice) pairs, a bound that some block reaches.
All inputs are finite; a program needn't handle non-finite values.
Results may differ from the reference program's by a relative error of at most 0.03.
Values may be sent and summed in bfloat16 or wider, within the bound.
A program may use at most 320 MiB of HBM per device.

```python
import math
import jax
import jax.numpy as jnp
import numpy as np
from jax import lax

D = 2048
HEADS = 16
NOPE = 128
ROPE = 64
VDIM = 128
KV_RANK = 512
HID = 1408
SHARED_HID = 2816
TOPK = 6
SEQ_LEN = 1024
SEQS_ALL = 8
TOK_DEV = 256
TOKENS = 8192
EXPERTS = 16
CAP = 192
N_MP = 4


def noise_array(key, marker, array_shape, fan_in):
    subkey = jax.random.fold_in(key, marker)
    values = jnp.clip(jax.random.normal(subkey, array_shape, jnp.float32), -4.0, 4.0)
    return values * fan_in ** (-0.5)


def draw_layer_input(key, part):
    values = noise_array(key, 11, (SEQS_ALL, SEQ_LEN, D), 1)
    return values.astype(jnp.bfloat16)


def draw_w_query(key, part):
    values = noise_array(key, 21, (D, HEADS * (NOPE + ROPE)), D)
    return values.astype(jnp.bfloat16)


def draw_w_latent(key, part):
    values = noise_array(key, 31, (D, KV_RANK + ROPE), D)
    return values.astype(jnp.bfloat16)


def draw_w_expand(key, part):
    values = noise_array(key, 41, (KV_RANK, HEADS * (NOPE + VDIM)), KV_RANK)
    return values.astype(jnp.bfloat16)


def block_scale(own_key, dims, split, least, top_value):
    level = 1.0
    for axis_at, shards_of in split:
        steps = jax.random.uniform(jax.random.fold_in(jax.random.fold_in(own_key, 6), axis_at), (shards_of,), jnp.float32, least / len(split), top_value / len(split))
        level = level * jnp.repeat(jnp.exp(steps), dims[axis_at] // shards_of).reshape((-1,) + (1,) * (len(dims) - 1 - axis_at))
    return level


def deal_out(rng, own, number, rows, number_of, top, most, lean):
    ranking = jax.random.permutation(rng, number_of)
    crowded, usual = load_shares(number_of, rows * top, most, lean, True), load_shares(number_of, rows * top, most, lean, False)
    places = jnp.arange(number_of)

    def named(sizes, turn):
        used = int((sizes > 0).sum())
        fixed = max(1, used // 4)
        moved = fixed + (places - fixed + turn * (used - fixed)) % max(1, number_of - fixed)
        return jnp.zeros((number_of,), jnp.int32).at[ranking[jnp.where(places < fixed, places, moved)]].set(jnp.asarray(sizes, jnp.int32))

    sizes = jnp.where(number % 4 == 0, named(crowded, number // 4), named(usual, number - number // 4 - 1))
    mixed = jax.random.permutation(jax.random.fold_in(own, 3), number_of)
    source_of, receiver = mixed[0:number_of // 2 * 2:2], mixed[1:number_of // 2 * 2:2]
    slack = jnp.minimum(sizes[source_of] - 1, most - sizes[receiver]) // 2
    slack = jnp.where((source_of == ranking[0]) | (receiver == ranking[0]) | (sizes[receiver] == 0), 0, jnp.maximum(slack, 0))
    moved = jax.random.randint(jax.random.fold_in(own, 4), (number_of // 2,), 0, 1 << 20) % (slack + 1)
    sizes = sizes.at[source_of].add(-moved).at[receiver].add(moved)
    members = jnp.searchsorted(jnp.cumsum(sizes), jnp.arange(rows * top), side="right").astype(jnp.int32)
    listing = members.reshape(top, rows).T
    listing = listing[jax.random.permutation(jax.random.fold_in(own, 1), rows)]
    turn = jax.random.randint(jax.random.fold_in(own, 2), (rows, 1), 0, top)
    return jnp.take_along_axis(listing, (jnp.arange(top)[None, :] + turn) % top, axis=1)


def load_shares(count, total, limit, lean, full):
    portions = [(1 << 20) // math.isqrt(grade ** lean) + 1 for grade in range(1, count + 1)]
    largest = limit if full else min(limit, max(-(-total // count), total * portions[0] // sum(portions)))
    least = 1 if total - largest >= count - 1 else 0
    holding, surplus = [largest] + [least] * (count - 1), total - largest - least * (count - 1)
    while surplus > 0:
        movable = [i for i in range(1, count) if holding[i] < largest] or [i for i in range(1, count) if holding[i] < limit]
        pool, remaining = sum([portions[i] for i in movable]), surplus
        for i in movable:
            more = min(limit - holding[i], max(1, remaining * portions[i] // pool), surplus)
            holding[i] = holding[i] + more
            surplus = surplus - more
    return np.array(holding)


def scatter_about(own_key, shape, width, bound, cuts=(), held_as=jnp.bfloat16):
    gain = block_scale(own_key, shape, cuts, -0.22, 0.18) if cuts else 1.0
    drawn = jax.random.normal(own_key, shape, jnp.float32) * width * gain
    return jnp.minimum(jnp.maximum(drawn, -bound), bound).astype(held_as)


def setup_inputs(seed: int = 0) -> dict:
    key_list = jax.random.split(jax.random.key(seed), 18)
    layer_input = draw_layer_input(jax.random.fold_in(key_list[17], 71), 0)
    w_query = draw_w_query(jax.random.fold_in(key_list[17], 71), 0)
    w_latent = draw_w_latent(jax.random.fold_in(key_list[17], 71), 0)
    latent_gain = jnp.clip(1.0 + 0.1 * jax.random.normal(key_list[3], (KV_RANK,), jnp.float32), 0.5, 1.5)
    w_expand = draw_w_expand(jax.random.fold_in(key_list[17], 71), 0)
    w_output = scatter_about(key_list[5], (HEADS * VDIM, D), (HEADS * VDIM // 32) ** -0.5, 0.75, ((0, 4), (1, 8)))
    attn_gain = jnp.clip(1.0 + 0.1 * jax.random.normal(key_list[6], (D,), jnp.float32), 0.5, 1.5)
    ffn_gain = jnp.clip(1.0 + 0.1 * jax.random.normal(key_list[7], (D,), jnp.float32), 0.5, 1.5)
    shared_gate = scatter_about(key_list[8], (D, SHARED_HID), D ** -0.5, 0.125, ((0, 8), (1, 4)))
    shared_up = scatter_about(key_list[9], (D, SHARED_HID), D ** -0.5, 0.125, ((0, 8), (1, 4)))
    shared_down = scatter_about(key_list[10], (SHARED_HID, D), SHARED_HID ** -0.5, 0.109375, ((0, 4), (1, 8)))
    expert_gate = scatter_about(key_list[11], (EXPERTS, D, HID), D ** -0.5, 0.125, ((0, 16), (1, 2)))
    expert_up = scatter_about(key_list[12], (EXPERTS, D, HID), D ** -0.5, 0.125, ((0, 16), (1, 2)))
    expert_down = scatter_about(key_list[13], (EXPERTS, HID, D), HID ** -0.5, 0.15625, ((0, 16), (2, 2)))
    routes_keys = jax.random.split(jax.random.fold_in(key_list[14], 1), SEQS_ALL * SEQ_LEN // TOK_DEV)
    routes_turns = jax.random.permutation(jax.random.fold_in(key_list[14], 3), SEQS_ALL * SEQ_LEN // TOK_DEV)
    routes = jax.vmap(lambda own, number: deal_out(jax.random.fold_in(key_list[14], 2), own, number, TOK_DEV, EXPERTS, TOPK, CAP, 2))(routes_keys, routes_turns).reshape((SEQS_ALL, SEQ_LEN, TOPK))
    combine = jnp.clip(0.05 + 0.35 * jax.random.uniform(key_list[15], (SEQS_ALL, SEQ_LEN, TOPK), jnp.float32) ** block_scale(key_list[15], (SEQS_ALL, SEQ_LEN, TOPK), ((0, 8), (1, 4)), -0.2, 0.2), 0.05, 0.4)
    cotangent = scatter_about(key_list[16], (SEQS_ALL, SEQ_LEN, D), 1.0, 6.0, ((0, 8), (1, 4)))
    return {"layer_input": layer_input, "w_query": w_query, "w_latent": w_latent, "latent_gain": latent_gain, "w_expand": w_expand, "w_output": w_output, "attn_gain": attn_gain, "ffn_gain": ffn_gain, "shared_gate": shared_gate, "shared_up": shared_up, "shared_down": shared_down, "expert_gate": expert_gate, "expert_up": expert_up, "expert_down": expert_down, "routes": routes, "combine": combine, "cotangent": cotangent}


epsilon = 1e-06
theta_base = 50000.0
masked_value = -1e+30
highest = lax.Precision.HIGHEST

@jax.custom_vjp
def low(v):
    return lax.optimization_barrier(v.astype(jnp.bfloat16)).astype(jnp.float32)

@jax.custom_vjp
def low_back(v):
    return v

def low_keep(v):
    return (low(v), None)

def low_pass(kept, grad):
    return (grad,)

def back_keep(v):
    return (v, None)

def back_low(kept, grad):
    return (low(grad),)
low.defvjp(low_keep, low_pass)
low_back.defvjp(back_keep, back_low)

def exact_dot(left_side, right_side):
    return jnp.dot(left_side, right_side, precision=highest, preferred_element_type=jnp.float32)

def rms_norm(values, gain_vector):
    return values * lax.rsqrt(lax.optimization_barrier(jnp.mean(values * values, axis=-1, keepdims=True)) + epsilon) * gain_vector

def rotate(values, cosine, sine_part):
    halfway = values.shape[-1] // 2
    leading = values[..., :halfway]
    trailing = values[..., halfway:]
    return jnp.concatenate([leading * cosine - trailing * sine_part, trailing * cosine + leading * sine_part], axis=-1)

def angles(length):
    inverse_freq = theta_base ** (-jnp.arange(0, ROPE, 2, dtype=jnp.float32) / ROPE)
    phases = jnp.arange(length, dtype=jnp.float32)[:, None] * inverse_freq[None, :]
    return (jnp.cos(phases), jnp.sin(phases))

def attend(queries, key_vectors, value_vectors):
    block_rows = min(512, SEQ_LEN)
    block_count = SEQ_LEN // block_rows
    factor = (NOPE + ROPE) ** (-0.5)
    key_pos = jnp.arange(SEQ_LEN, dtype=jnp.int32)

    def one_block(operands):
        query_block, offset = operands
        scores = low_back(jnp.einsum('qhd,khd->hqk', query_block, key_vectors, precision=highest) * factor)
        query_pos = offset + jnp.arange(block_rows, dtype=jnp.int32)
        scores = jnp.where((key_pos[None, :] <= query_pos[:, None])[None], scores, masked_value)
        largest = lax.optimization_barrier(jnp.max(scores, axis=-1, keepdims=True))
        exponentials = jnp.exp(scores - largest)
        weights_low = low(exponentials / lax.optimization_barrier(jnp.sum(exponentials, axis=-1, keepdims=True)))
        return jnp.einsum('hqk,khd->qhd', weights_low, value_vectors, precision=highest)
    blocked = queries.reshape(block_count, block_rows, HEADS, NOPE + ROPE)
    offsets = jnp.arange(block_count, dtype=jnp.int32) * block_rows
    return lax.map(jax.checkpoint(one_block), (blocked, offsets)).reshape(SEQ_LEN, HEADS, VDIM)

def build_slots(routes, combine):
    block_total = SEQS_ALL * N_MP
    pair_total = TOK_DEV * TOPK
    chosen = routes.reshape(block_total, pair_total).astype(jnp.int32)
    one_hot = (chosen[:, :, None] == jnp.arange(EXPERTS, dtype=jnp.int32)[None, None, :]).astype(jnp.int32)
    ranks = lax.optimization_barrier(jnp.sum((jnp.cumsum(one_hot, axis=1) - 1) * one_hot, axis=2))
    slots = chosen * CAP + ranks
    tokens = jnp.arange(block_total, dtype=jnp.int32)[:, None] * TOK_DEV + jnp.arange(pair_total, dtype=jnp.int32)[None, :] // TOPK
    mixing = combine.reshape(block_total, pair_total).astype(jnp.float32)

    def fill_block(slot_row, token_row, mixing_row):
        table = jnp.full((EXPERTS * CAP,), TOKENS, jnp.int32).at[slot_row].set(token_row)
        scaled = jnp.zeros((EXPERTS * CAP,), jnp.float32).at[slot_row].set(mixing_row)
        return (table, scaled)
    table, scaled = jax.vmap(fill_block)(slots, tokens, mixing)
    table = table.reshape(block_total, EXPERTS, CAP).transpose(1, 0, 2).reshape(EXPERTS, block_total * CAP)
    scaled = scaled.reshape(block_total, EXPERTS, CAP).transpose(1, 0, 2).reshape(EXPERTS, block_total * CAP)
    return (table, scaled)

def layer_forward(layer_input, w_query, w_latent, latent_gain, w_expand, w_output, attn_gain, ffn_gain, shared_gate, shared_up, shared_down, expert_gate, expert_up, expert_down, table, scaled):
    cosine, sine_part = angles(SEQ_LEN)

    def sequence(inputs):
        normed = low(rms_norm(inputs, attn_gain))
        query_pre = low_back(exact_dot(normed, w_query)).reshape(SEQ_LEN, HEADS, NOPE + ROPE)
        queries = low(jnp.concatenate([query_pre[..., :NOPE], rotate(query_pre[..., NOPE:], cosine[:, None, :], sine_part[:, None, :])], axis=-1))
        latent_raw = low_back(exact_dot(normed, w_latent))
        latent = low(jnp.concatenate([rms_norm(latent_raw[:, :KV_RANK], latent_gain), rotate(latent_raw[:, KV_RANK:], cosine, sine_part)], axis=-1))
        expanded = low(low_back(exact_dot(latent[:, :KV_RANK], w_expand))).reshape(SEQ_LEN, HEADS, NOPE + VDIM)
        key_vectors = jnp.concatenate([expanded[..., :NOPE], jnp.broadcast_to(latent[:, None, KV_RANK:], (SEQ_LEN, HEADS, ROPE))], axis=-1)
        heads_raw = attend(queries, key_vectors, expanded[..., NOPE:]).reshape(SEQ_LEN, HEADS * VDIM)
        heads_out = low(low_back(heads_raw))
        return inputs + low_back(exact_dot(heads_out, w_output))
    residual = lax.map(jax.checkpoint(sequence), layer_input).reshape(TOKENS, D)
    ffn_in = low(rms_norm(residual, ffn_gain))
    gate_value = low_back(exact_dot(ffn_in, shared_gate))
    up_value = low_back(exact_dot(ffn_in, shared_up))
    shared_hidden = low(jax.nn.silu(gate_value) * up_value)
    shared_out = low_back(exact_dot(shared_hidden, shared_down))
    padded = jnp.concatenate([ffn_in, jnp.zeros((1, D), jnp.float32)], axis=0)

    def one_expert(operands):
        token_rows, mixing_row, gate_matrix, up_matrix, down_matrix = operands
        arrived = low_back(padded[token_rows])
        expert_gate_value = low_back(exact_dot(arrived, gate_matrix))
        expert_up_value = low_back(exact_dot(arrived, up_matrix))
        hidden = low(jax.nn.silu(expert_gate_value) * expert_up_value)
        return low(low_back(exact_dot(hidden, down_matrix))) * mixing_row[:, None]
    weighted = lax.map(jax.checkpoint(one_expert), (table, scaled, expert_gate, expert_up, expert_down))
    routed_out = jax.ops.segment_sum(weighted.reshape(-1, D), table.reshape(-1), num_segments=TOKENS + 1)[:TOKENS]
    return (residual + shared_out + routed_out).reshape(SEQS_ALL, SEQ_LEN, D)

def reference(layer_input, w_query, w_latent, latent_gain, w_expand, w_output, attn_gain, ffn_gain, shared_gate, shared_up, shared_down, expert_gate, expert_up, expert_down, routes, combine, cotangent):
    table, scaled = build_slots(routes, combine)
    params = (layer_input, w_query, w_latent, latent_gain, w_expand, w_output, attn_gain, ffn_gain, shared_gate, shared_up, shared_down, expert_gate, expert_up, expert_down)
    params = tuple((value.astype(jnp.float32) for value in params))

    def forward(*inputs):
        return layer_forward(*inputs, table, scaled)
    result, pullback = jax.vjp(forward, *params)
    grads = pullback(cotangent.astype(jnp.float32))
    return (result, grads[0], grads[1], grads[2], grads[3], grads[4], grads[5], grads[6], grads[7], grads[8], grads[9], grads[10], grads[11], grads[12], grads[13])
```

```python
import jax
import jax.numpy as jnp
from jax import lax
from jax.sharding import PartitionSpec as P

NOPE = 128
ROPE = 64
VDIM = 128
KV_RANK = 512
TOPK = 6


epsilon = 1e-06
theta_base = 50000.0
masked_value = -1e30


def rms_norm(values, gain_vector):
    return (
        values
        * lax.rsqrt(jnp.mean(values * values, axis=-1, keepdims=True) + epsilon)
        * gain_vector
    )


def norm_back(values, gain_vector, upstream):
    inverse = lax.rsqrt(jnp.mean(values * values, axis=-1, keepdims=True) + epsilon)
    normed = values * inverse
    scaled = upstream * gain_vector
    d_values = inverse * (scaled - normed * jnp.mean(scaled * normed, axis=-1, keepdims=True))
    return (d_values, jnp.sum(upstream * normed, axis=0))


def rotate(values, cosine, sine_part):
    halfway = values.shape[-1] // 2
    leading = values[..., :halfway]
    trailing = values[..., halfway:]
    return jnp.concatenate(
        [leading * cosine - trailing * sine_part, trailing * cosine + leading * sine_part], axis=-1
    )


def angles(length):
    inverse_freq = theta_base ** (-jnp.arange(0, ROPE, 2, dtype=jnp.float32) / ROPE)
    phases = jnp.arange(length, dtype=jnp.float32)[:, None] * inverse_freq[None, :]
    return (jnp.cos(phases), jnp.sin(phases))


def product(left_side, right_side):
    return jnp.dot(left_side, right_side, preferred_element_type=jnp.float32)


def left_product(left_side, right_side):
    return lax.dot_general(
        left_side, right_side, (((0,), (0,)), ((), ())), preferred_element_type=jnp.float32
    )


def right_product(left_side, right_side):
    return lax.dot_general(
        left_side, right_side, (((1,), (1,)), ((), ())), preferred_element_type=jnp.float32
    )


def silu_grads(gate_value, up_value, upstream):
    sigmoid = jax.nn.sigmoid(gate_value)
    gate_grad = upstream * up_value * sigmoid * (1.0 + gate_value * (1.0 - sigmoid))
    up_grad = upstream * gate_value * sigmoid
    return (gate_grad.astype(jnp.bfloat16), up_grad.astype(jnp.bfloat16))


def causal_mask(offset, block_rows, key_span):
    query_pos = offset + jnp.arange(block_rows, dtype=jnp.int32)
    key_pos = jnp.arange(key_span, dtype=jnp.int32)
    return (key_pos[None, :] <= query_pos[:, None])[None]


def full_rows(values):
    return lax.all_gather(values, "mp", axis=0, tiled=True)


def summed_rows(term, row_count):
    return lax.psum_scatter(
        term(jnp.int32(0), row_count * lax.axis_size("mp")).astype(jnp.bfloat16),
        "mp",
        scatter_dimension=0,
        tiled=True,
    ).astype(jnp.float32)


def partner(values, axis, mask):
    size = lax.axis_size(axis)
    return lax.ppermute(values, axis, [(index, index ^ mask) for index in range(size)])


def relative_blocks(values):
    blocks = [values]
    mask = 1
    while mask < lax.axis_size("expert"):
        mask *= 2
    while mask > 1:
        mask //= 2
        blocks = blocks + [partner(block, "expert", mask) for block in blocks]
    size = lax.axis_size("expert")
    order = [0]
    mask = size
    while mask > 1:
        mask //= 2
        order = order + [index ^ mask for index in order]
    return [blocks[order.index(index)] for index in range(size)]


def relative_sum(blocks):
    size = len(blocks)
    kept = dict(enumerate(blocks))
    mask = 1
    while mask < size:
        moved = {index: partner(kept[index], "expert", mask) for index in kept if index & mask}
        kept = {
            index: kept[index].astype(jnp.float32) + moved[index ^ mask].astype(jnp.float32)
            for index in kept
            if not index & mask
        }
        mask *= 2
        if mask < size:
            kept = {index: kept[index].astype(jnp.bfloat16) for index in kept}
    return kept[0]


def whole_weight(shard, axis):
    if lax.axis_size("dp") != 2:
        return lax.all_gather(shard, "dp", axis=axis, tiled=True)
    other = partner(shard, "dp", 1)
    first = lax.axis_index("dp") == 0
    return jnp.concatenate(
        [jnp.where(first, shard, other), jnp.where(first, other, shard)], axis=axis
    )


def summed_weight(partial, axis):
    if lax.axis_size("dp") != 2:
        return lax.psum_scatter(
            partial.astype(jnp.bfloat16), "dp", scatter_dimension=axis, tiled=True
        ).astype(jnp.float32)
    half = partial.shape[axis] // 2
    position = lax.axis_index("dp")
    partial = partial.astype(jnp.bfloat16)
    leaving = lax.dynamic_slice_in_dim(partial, (1 - position) * half, half, axis)
    staying = lax.dynamic_slice_in_dim(partial, position * half, half, axis)
    arrived = partner(leaving, "dp", 1)
    return staying.astype(jnp.float32) + arrived.astype(jnp.float32)


def local(
    layer_input,
    w_query,
    w_latent,
    latent_gain,
    w_expand,
    w_output,
    attn_gain,
    ffn_gain,
    shared_gate,
    shared_up,
    shared_down,
    expert_gate,
    expert_up,
    expert_down,
    routes,
    combine,
    cotangent,
):
    row_count = layer_input.shape[1]
    width = layer_input.shape[2]
    seq_len = row_count * lax.axis_size("mp")
    first_row = lax.axis_index("mp") * row_count
    head_dim = NOPE + ROPE
    factor = head_dim ** (-0.5)
    head_count = w_query.shape[1] // head_dim
    block_rows = min(512, seq_len)
    block_count = seq_len // block_rows
    query_whole, expand_whole, output_whole, gate_whole, up_whole, down_whole = (
        lax.all_gather(w_query, ("dp", "expert"), axis=0, tiled=True),
        lax.all_gather(w_expand, ("dp", "expert"), axis=0, tiled=True),
        lax.all_gather(w_output, ("dp", "expert"), axis=1, tiled=True),
        lax.all_gather(shared_gate, ("dp", "expert"), axis=0, tiled=True),
        lax.all_gather(shared_up, ("dp", "expert"), axis=0, tiled=True),
        lax.all_gather(shared_down, ("dp", "expert"), axis=1, tiled=True),
    )
    latent_whole = lax.all_gather(w_latent, ("dp", "mp", "expert"), axis=0, tiled=True)
    cosine_all, sine_all = angles(seq_len)
    cosine_own = lax.dynamic_slice_in_dim(cosine_all, first_row, row_count, 0)
    sine_own = lax.dynamic_slice_in_dim(sine_all, first_row, row_count, 0)
    inputs_own = layer_input[0].astype(jnp.float32)
    normed_own = rms_norm(inputs_own, attn_gain).astype(jnp.bfloat16)
    latent_raw = product(normed_own, latent_whole)
    latent_own = jnp.concatenate(
        [
            rms_norm(latent_raw[:, :KV_RANK], latent_gain),
            rotate(latent_raw[:, KV_RANK:], cosine_own, sine_own),
        ],
        axis=1,
    ).astype(jnp.bfloat16)
    normed_all = full_rows(normed_own)
    latent_all = full_rows(latent_own)
    query_pre = product(normed_all, query_whole).reshape(seq_len, head_count, head_dim)
    queries = jnp.concatenate(
        [
            query_pre[..., :NOPE],
            rotate(query_pre[..., NOPE:], cosine_all[:, None, :], sine_all[:, None, :]),
        ],
        axis=-1,
    ).astype(jnp.bfloat16)
    expanded = (
        product(latent_all[:, :KV_RANK], expand_whole)
        .astype(jnp.bfloat16)
        .reshape(seq_len, head_count, NOPE + VDIM)
    )
    key_vectors = jnp.concatenate(
        [
            expanded[..., :NOPE],
            jnp.broadcast_to(latent_all[:, None, KV_RANK:], (seq_len, head_count, ROPE)),
        ],
        axis=-1,
    )
    value_vectors = expanded[..., NOPE:]
    pieces = []
    maxima = []
    totals = []
    for block_index in range(block_count):
        lower = block_index * block_rows
        key_span = lower + block_rows
        scores = (
            jnp.einsum(
                "qhd,khd->hqk",
                queries[lower:key_span],
                key_vectors[:key_span],
                preferred_element_type=jnp.float32,
            )
            * factor
        )
        scores = jnp.where(causal_mask(lower, block_rows, key_span), scores, masked_value)
        largest = jnp.max(scores, axis=-1, keepdims=True)
        exponentials = jnp.exp(scores - largest)
        row_total = jnp.sum(exponentials, axis=-1, keepdims=True)
        weights_low = (exponentials / row_total).astype(jnp.bfloat16)
        pieces.append(
            jnp.einsum(
                "hqk,khd->qhd",
                weights_low,
                value_vectors[:key_span],
                preferred_element_type=jnp.float32,
            )
        )
        maxima.append(largest)
        totals.append(row_total)
    heads_raw = jnp.concatenate(pieces, axis=0)
    heads_out = heads_raw.astype(jnp.bfloat16).reshape(seq_len, head_count * VDIM)

    def attention_term(offset, length):
        return product(heads_out, output_whole)

    residual = inputs_own + summed_rows(attention_term, row_count)
    ffn_in = rms_norm(residual, ffn_gain).astype(jnp.bfloat16)
    ffn_all = full_rows(ffn_in)
    shared_gate_value = product(ffn_all, gate_whole)
    shared_up_value = product(ffn_all, up_whole)
    shared_hidden = (jax.nn.silu(shared_gate_value) * shared_up_value).astype(jnp.bfloat16)

    expert_total = lax.axis_size(("mp", "expert"))
    capacity = max(2, (2 * row_count * TOPK + expert_total - 1) // expert_total)
    position_count = lax.axis_size("mp")
    group_count = lax.axis_size("expert")
    block_total = position_count * group_count
    own_group = lax.axis_index("expert")
    own_expert = lax.axis_index("mp") * group_count + own_group
    mixing_table = jnp.sum(
        jnp.where(
            routes[0][None] == jnp.arange(expert_total, dtype=jnp.int32)[:, None, None],
            combine[0][None],
            0.0,
        ),
        axis=2,
    )
    mixing_all = lax.all_gather(mixing_table, ("mp", "expert"), axis=0).reshape(
        position_count, group_count, expert_total, row_count
    )
    mixing_own = lax.dynamic_index_in_dim(mixing_all, own_expert, 2, keepdims=False)
    mixing = jnp.concatenate(
        [
            lax.dynamic_index_in_dim(mixing_own, own_group ^ index, 1, keepdims=False)
            for index in range(group_count)
        ],
        axis=0,
    )
    chosen = mixing > 0.0
    earlier = jnp.triu(jnp.ones((row_count, row_count), jnp.bfloat16), 1)
    ranks = product(chosen.astype(jnp.bfloat16), earlier).astype(jnp.int32)
    picks = chosen[:, None, :] & (
        ranks[:, None, :] == jnp.arange(capacity, dtype=jnp.int32)[None, :, None]
    )
    slot_mixing = jnp.sum(jnp.where(picks, mixing[:, None, :], 0.0), axis=2)
    slot_mixing = slot_mixing.reshape(block_total * capacity, 1)
    picks = picks.astype(jnp.bfloat16)

    def dispatch(gathered):
        blocks = jnp.concatenate(
            [
                block.reshape(position_count, row_count, width)
                for block in relative_blocks(gathered)
            ],
            axis=0,
        )
        return jnp.einsum(
            "bct,btd->bcd", picks, blocks, preferred_element_type=jnp.bfloat16
        ).reshape(block_total * capacity, width)

    def collect(rows):
        partial = jnp.einsum(
            "bct,bcd->btd",
            picks,
            rows.reshape(block_total, capacity, width),
            preferred_element_type=jnp.bfloat16,
        ).reshape(group_count, seq_len, width)
        return relative_sum([partial[index] for index in range(group_count)])

    gate_expert = whole_weight(expert_gate[0], 0)
    up_expert = whole_weight(expert_up[0], 0)
    down_expert = whole_weight(expert_down[0], 1)
    upstream_own = cotangent[0].astype(jnp.float32)
    upstream_all = full_rows(cotangent[0])
    arrived_grads = (dispatch(upstream_all).astype(jnp.float32) * slot_mixing).astype(jnp.bfloat16)
    arrived_in = dispatch(ffn_all)
    expert_gate_value = product(arrived_in, gate_expert)
    expert_up_value = product(arrived_in, up_expert)
    expert_hidden = (jax.nn.silu(expert_gate_value) * expert_up_value).astype(jnp.bfloat16)
    hidden_grad = right_product(arrived_grads, down_expert)
    gate_grad_e, up_grad_e = silu_grads(expert_gate_value, expert_up_value, hidden_grad)
    input_grads = (
        right_product(gate_grad_e, gate_expert) + right_product(up_grad_e, up_expert)
    ).astype(jnp.bfloat16)
    routed_back = collect(input_grads)
    expert_result = (slot_mixing * product(expert_hidden, down_expert)).astype(jnp.bfloat16)
    routed_out = collect(expert_result)

    def output_term(offset, length):
        return product(shared_hidden, down_whole) + routed_out

    output_own = residual + summed_rows(output_term, row_count)
    grad_gate_e, grad_up_e, grad_down_e = (
        summed_weight(left_product(arrived_in, gate_grad_e), 0)[None],
        summed_weight(left_product(arrived_in, up_grad_e), 0)[None],
        summed_weight(left_product(expert_hidden, arrived_grads), 1)[None],
    )
    shared_hidden_grad = right_product(upstream_all, down_whole)
    grad_shared_down = left_product(shared_hidden, upstream_all)
    shared_gate_grad, shared_up_grad = silu_grads(
        shared_gate_value, shared_up_value, shared_hidden_grad
    )
    grad_shared_gate = left_product(ffn_all, shared_gate_grad)
    grad_shared_up = left_product(ffn_all, shared_up_grad)

    def shared_back_term(offset, length):
        return (
            right_product(shared_gate_grad, gate_whole)
            + right_product(shared_up_grad, up_whole)
            + routed_back
        )

    ffn_grad = summed_rows(shared_back_term, row_count)
    residual_part, grad_ffn_gain = norm_back(residual, ffn_gain, ffn_grad)
    residual_grad = upstream_own + residual_part
    residual_all = full_rows(residual_grad.astype(jnp.bfloat16))
    grad_output_w = left_product(heads_out, residual_all)
    heads_grad = (
        right_product(residual_all, output_whole)
        .astype(jnp.bfloat16)
        .reshape(seq_len, head_count, VDIM)
    )
    row_delta = jnp.sum(heads_grad.astype(jnp.float32) * heads_raw, axis=-1)
    query_pieces = []
    key_grad = jnp.zeros((seq_len, head_count, head_dim), jnp.float32)
    value_grad = jnp.zeros((seq_len, head_count, VDIM), jnp.float32)
    for block_index in range(block_count):
        lower = block_index * block_rows
        key_span = lower + block_rows
        query_block = queries[lower:key_span]
        grad_block = heads_grad[lower:key_span]
        scores = (
            jnp.einsum(
                "qhd,khd->hqk",
                query_block,
                key_vectors[:key_span],
                preferred_element_type=jnp.float32,
            )
            * factor
        )
        scores = jnp.where(causal_mask(lower, block_rows, key_span), scores, masked_value)
        weights_full = jnp.exp(scores - maxima[block_index]) / totals[block_index]
        weights_low = weights_full.astype(jnp.bfloat16)
        value_grad = value_grad.at[:key_span].add(
            jnp.einsum("hqk,qhd->khd", weights_low, grad_block, preferred_element_type=jnp.float32)
        )
        weight_grad = jnp.einsum(
            "qhd,khd->hqk", grad_block, value_vectors[:key_span], preferred_element_type=jnp.float32
        )
        delta_block = jnp.transpose(row_delta[lower:key_span])[:, :, None]
        score_grad = (weights_full * (weight_grad - delta_block)).astype(jnp.bfloat16)
        query_pieces.append(
            jnp.einsum(
                "hqk,khd->qhd",
                score_grad,
                key_vectors[:key_span],
                preferred_element_type=jnp.float32,
            )
            * factor
        )
        key_grad = key_grad.at[:key_span].add(
            jnp.einsum("hqk,qhd->khd", score_grad, query_block, preferred_element_type=jnp.float32)
            * factor
        )
    query_grad = jnp.concatenate(query_pieces, axis=0)
    query_grad = jnp.concatenate(
        [
            query_grad[..., :NOPE],
            rotate(query_grad[..., NOPE:], cosine_all[:, None, :], -sine_all[:, None, :]),
        ],
        axis=-1,
    )
    query_grad = query_grad.astype(jnp.bfloat16).reshape(seq_len, head_count * head_dim)
    rope_grad = jnp.sum(key_grad[..., NOPE:], axis=1)
    expand_grad = (
        jnp.concatenate([key_grad[..., :NOPE], value_grad], axis=-1)
        .astype(jnp.bfloat16)
        .reshape(seq_len, head_count * (NOPE + VDIM))
    )
    grad_query_w = left_product(normed_all, query_grad)
    grad_expand_w = left_product(latent_all[:, :KV_RANK], expand_grad)

    def query_term(offset, length):
        return right_product(query_grad, query_whole)

    def latent_term(offset, length):
        return jnp.concatenate([right_product(expand_grad, expand_whole), rope_grad], axis=1)

    normed_grad = summed_rows(query_term, row_count)
    latent_grad = summed_rows(latent_term, row_count)
    compress_grad, grad_latent_gain = norm_back(
        latent_raw[:, :KV_RANK], latent_gain, latent_grad[:, :KV_RANK]
    )
    rope_back = rotate(latent_grad[:, KV_RANK:], cosine_own, -sine_own)
    latent_raw_grad = jnp.concatenate([compress_grad, rope_back], axis=1).astype(jnp.bfloat16)
    dp_count = lax.axis_size("dp")
    grad_latent_w = (
        left_product(normed_own, latent_raw_grad)
        .reshape(dp_count, position_count, group_count, -1, latent_raw_grad.shape[1])
        .transpose(0, 2, 1, 3, 4)
        .reshape(width, latent_raw_grad.shape[1])
    )
    normed_grad = normed_grad + right_product(latent_raw_grad, latent_whole)
    input_part, grad_attn_gain = norm_back(inputs_own, attn_gain, normed_grad)
    input_grad = residual_grad + input_part
    (
        grad_query_w,
        grad_expand_w,
        grad_output_w,
        grad_shared_gate,
        grad_shared_up,
        grad_shared_down,
    ) = (
        lax.psum_scatter(
            grad_query_w.astype(jnp.bfloat16), ("dp", "expert"), scatter_dimension=0, tiled=True
        ).astype(jnp.float32),
        lax.psum_scatter(
            grad_expand_w.astype(jnp.bfloat16), ("dp", "expert"), scatter_dimension=0, tiled=True
        ).astype(jnp.float32),
        lax.psum_scatter(
            grad_output_w.astype(jnp.bfloat16), ("dp", "expert"), scatter_dimension=1, tiled=True
        ).astype(jnp.float32),
        lax.psum_scatter(
            grad_shared_gate.astype(jnp.bfloat16), ("dp", "expert"), scatter_dimension=0, tiled=True
        ).astype(jnp.float32),
        lax.psum_scatter(
            grad_shared_up.astype(jnp.bfloat16), ("dp", "expert"), scatter_dimension=0, tiled=True
        ).astype(jnp.float32),
        lax.psum_scatter(
            grad_shared_down.astype(jnp.bfloat16), ("dp", "expert"), scatter_dimension=1, tiled=True
        ).astype(jnp.float32),
    )
    grad_latent_w = lax.psum_scatter(
        grad_latent_w.astype(jnp.bfloat16), ("dp", "expert"), scatter_dimension=0, tiled=True
    )
    grad_latent_w = lax.psum_scatter(
        grad_latent_w, "mp", scatter_dimension=0, tiled=True
    ).astype(jnp.float32)
    grad_attn_gain, grad_ffn_gain, grad_latent_gain = lax.psum(
        (grad_attn_gain, grad_ffn_gain, grad_latent_gain), ("dp", "mp", "expert")
    )
    return (
        output_own[None],
        input_grad[None],
        grad_query_w,
        grad_latent_w,
        grad_latent_gain,
        grad_expand_w,
        grad_output_w,
        grad_attn_gain,
        grad_ffn_gain,
        grad_shared_gate,
        grad_shared_up,
        grad_shared_down,
        grad_gate_e,
        grad_up_e,
        grad_down_e,
    )


def solution(mesh):
    placed = (
        P(("dp", "expert"), "mp", None),
        P(("dp", "expert"), "mp"),
        P(("dp", "mp", "expert"), None),
        P(),
        P(("dp", "expert"), "mp"),
        P("mp", ("dp", "expert")),
        P(),
        P(),
        P(("dp", "expert"), "mp"),
        P(("dp", "expert"), "mp"),
        P("mp", ("dp", "expert")),
        P(("mp", "expert"), "dp", None),
        P(("mp", "expert"), "dp", None),
        P(("mp", "expert"), None, "dp"),
        P(("dp", "expert"), "mp", None),
        P(("dp", "expert"), "mp", None),
        P(("dp", "expert"), "mp", None),
    )
    return jax.shard_map(
        local,
        mesh=mesh,
        in_specs=placed,
        out_specs=(
            P(("dp", "expert"), "mp", None),
            P(("dp", "expert"), "mp", None),
            P(("dp", "expert"), "mp"),
            P(("dp", "mp", "expert"), None),
            P(),
            P(("dp", "expert"), "mp"),
            P("mp", ("dp", "expert")),
            P(),
            P(),
            P(("dp", "expert"), "mp"),
            P(("dp", "expert"), "mp"),
            P("mp", ("dp", "expert")),
            P(("mp", "expert"), "dp", None),
            P(("mp", "expert"), "dp", None),
            P(("mp", "expert"), None, "dp"),
        ),
        check_vma=False,
    )
```
